32 devices in a mesh: tm: 8 (over z, y), space: 4 (over x, core).
Axes of the slice: x: 2, y: 2, z: 4, core: 2. Of those that a mesh axis runs over, the one named last changes fastest.
Arguments:
- starts: float32 [8, 5, 16, 64, 128], P('tm', None, 'space'), may hold values from -4 to 4
- source: float32 [5, 16, 64, 128], P(None, 'space'), may hold values from -4 to 4
Outputs:
- ends: float32 [8, 5, 16, 64, 128], P('tm', None, 'space')
- slice_norms: float32 [8], P('tm')
- total_norm: float32 [1], replicated
The draws below stay inside these ranges and needn't reach their ends.
All inputs are finite; a program needn't handle non-finite values.
Results may differ from the reference program's by a relative error of at most 0.0003.
Values sent between devices are 32-bit elements; how exact they have to be, the bound alone decides.
A program may use at most 64 MiB of HBM per device.

```python
import math
import jax
import jax.numpy as jnp
from jax import lax

FIELDS = 5
NX = 128
NY = 64
STEPS = 1
NZ = 16
SLICES = 8


def block_levels(rng, dims, cuts, least, top_value):
    gain, own = 1.0, jax.random.fold_in(rng, 6)
    for position, parts in cuts:
        draws = jnp.exp(jax.random.uniform(jax.random.fold_in(own, position), (parts,), jnp.float32, least / len(cuts), top_value / len(cuts)))
        gain = gain * jnp.repeat(draws, dims[position] // parts).reshape([-1 if axis == position else 1 for axis in range(len(dims))])
    return gain


def normal_values(stream_key, extent, deviation, reach, split=(), kind=jnp.bfloat16):
    entries = jax.random.normal(stream_key, extent, jnp.float32) * deviation
    if len(split) > 0:
        entries = block_levels(stream_key, extent, split, -0.22, 0.18) * entries
    return jnp.clip(entries, min=-reach, max=reach).astype(kind)


def setup_inputs(seed: int = 0) -> dict:
    key_of = jax.random.split(jax.random.key(seed), 3)
    return {
        "starts": normal_values(key_of[0], (SLICES, FIELDS, NZ, NY, NX), 0.3, 4.0, ((0, 8), (2, 4)), jnp.float32),
        "source": normal_values(key_of[1], (FIELDS, NZ, NY, NX), 0.3, 4.0, ((1, 4),), jnp.float32),
    }


viscosity = 0.08
diffusivity = 0.05
compress_rate = 0.25
time_step = 0.5
diffusion_number = 0.08
advect_xaxis = 0.2
advect_yaxis = 0.15
advect_zaxis = 0.1
epsilon = 1e-06

def central(values, axis):
    return 0.5 * (jnp.roll(values, -1, axis) - jnp.roll(values, 1, axis))

def laplace(values):
    summed = -6.0 * values
    for axis in (0, 1, 2):
        summed = summed + jnp.roll(values, -1, axis) + jnp.roll(values, 1, axis)
    return summed

def tendency(state_now, source):
    speed_xaxis = advect_xaxis + state_now[0]
    speed_yaxis = advect_yaxis + state_now[1]
    speed_zaxis = advect_zaxis + state_now[2]

    def transport(quantity):
        return central(speed_xaxis * quantity, 2) + central(speed_yaxis * quantity, 1) + central(speed_zaxis * quantity, 0)
    pressure = state_now[3]
    xmomentum = -transport(state_now[0]) - central(pressure, 2) + viscosity * laplace(state_now[0])
    ymomentum = -transport(state_now[1]) - central(pressure, 1) + viscosity * laplace(state_now[1])
    zmomentum = -transport(state_now[2]) - central(pressure, 0) + viscosity * laplace(state_now[2])
    pressure_rate = -compress_rate * (central(state_now[0], 2) + central(state_now[1], 1) + central(state_now[2], 0))
    scalar_rate = -transport(state_now[4]) + diffusivity * laplace(state_now[4])
    return jnp.stack([xmomentum, ymomentum, zmomentum, pressure_rate, scalar_rate]) + source

def fine_run(current, source):
    for repeat in range(STEPS):
        section_one = tendency(current, source)
        section_two = tendency(current + 0.5 * time_step * section_one, source)
        section_three = tendency(current + 0.5 * time_step * section_two, source)
        section_four = tendency(current + time_step * section_three, source)
        current = current + time_step / 6.0 * (section_one + 2.0 * section_two + 2.0 * section_three + section_four)
    return current

def signed_angle(length):
    cell_ids = jnp.arange(length, dtype=jnp.int32)
    signed = (cell_ids + length // 2) % length - length // 2
    return (signed, 2.0 * math.pi / length * signed.astype(jnp.float32))

def coarse_symbol():
    zsigned, zangles = signed_angle(NZ)
    ysigned, yangles = signed_angle(NY)
    xsigned, xangles = signed_angle(NX)
    keeper = ((jnp.abs(ysigned) < NY // 8)[:, None] & (jnp.abs(xsigned) < NX // 16)[None, :]).astype(jnp.float32)
    real_part = 1.0 + diffusion_number * ((2.0 * jnp.cos(zangles) - 2.0)[:, None, None] + (2.0 * jnp.cos(yangles) - 2.0)[None, :, None] + (2.0 * jnp.cos(xangles) - 2.0)[None, None, :])
    imag_part = -(advect_zaxis * jnp.sin(zangles)[:, None, None] + advect_yaxis * jnp.sin(yangles)[None, :, None] + advect_xaxis * jnp.sin(xangles)[None, None, :])
    return lax.complex(real_part * keeper[None], imag_part * keeper[None])

def coarse(values, symbol):
    spectrum = jnp.fft.fftn(values, axes=(1, 2, 3))
    return jnp.real(jnp.fft.ifftn(spectrum * symbol, axes=(1, 2, 3)))

def reference(starts, source):

    def run_slice(begin_state):
        return fine_run(begin_state, source)
    fine = lax.map(run_slice, starts)
    symbol = coarse_symbol()

    def advance(carried, inputs_pair):
        old_start, fine_end = inputs_pair
        end_state = fine_end + coarse(carried - old_start, symbol)
        jump_size = end_state - fine_end
        return (end_state, (end_state, jnp.sum(jump_size * jump_size)))
    unused, (ends, sums) = lax.scan(advance, starts[0], (starts, fine))
    cell_total = FIELDS * NZ * NY * NX
    slice_norms = jnp.sqrt(sums / cell_total + epsilon)
    total_norm = jnp.sqrt(jnp.sum(sums) / (cell_total * SLICES) + epsilon).reshape(1)
    return (ends, slice_norms, total_norm)
```

```python
import functools
import math

import jax
import jax.numpy as jnp
import numpy as np
from jax import lax
from jax.experimental import pallas as pl
from jax.experimental.pallas import tpu as pltpu
from jax.sharding import PartitionSpec as P

viscosity = 0.08
diffusivity = 0.05
compress_rate = 0.25
time_step = 0.5
diffusion_number = 0.08
advect_xaxis = 0.2
advect_yaxis = 0.15
advect_zaxis = 0.1
epsilon = 1e-06
MESH = pl.DeviceIdType.MESH
PAD = 8
CHUNK = 16
LANES = 128


def tables(depth, rows, cols, spaces):
    keep_y, keep_x = rows // 8, cols // 16
    slot = 2 * keep_x
    per = LANES // (slot * depth)
    full = depth * spaces
    k = np.arange(keep_x)
    x = np.arange(cols)
    ax = 2 * math.pi / cols * ((x[:, None] * k[None, :]) % cols)
    weight = np.where(k == 0, 1.0, 2.0) / (full * rows * cols)
    xf = np.zeros((2 * cols, LANES))
    xi = np.zeros((LANES, 2 * cols))
    for i in range(2):
        at = i * slot
        xf[i * cols : (i + 1) * cols, at : at + keep_x] = np.cos(ax)
        xf[i * cols : (i + 1) * cols, at + keep_x : at + slot] = -np.sin(ax)
        xi[at : at + keep_x, i * cols : (i + 1) * cols] = (np.cos(ax) * weight).T
        xi[at + keep_x : at + slot, i * cols : (i + 1) * cols] = (-np.sin(ax) * weight).T
    ky = np.arange(2 * keep_y)
    ky = np.where(ky < keep_y, ky, ky - 2 * keep_y)
    y = np.arange(rows)
    ay = 2 * math.pi / rows * ((ky[:, None] * y[None, :]) % rows)
    yf = np.concatenate([np.cos(ay), np.sin(ay)], axis=1)
    yi = np.concatenate([np.cos(ay).T, -np.sin(ay).T], axis=1)
    kz = np.arange(full)
    width = full * keep_x
    half = depth * slot
    zf = np.zeros((LANES, per * 2 * width))
    for fp in range(per):
        for z in range(depth):
            a = 2 * math.pi / full * ((kz * z) % full)
            for kk in range(keep_x):
                row = fp * half + z * slot + kk
                re = fp * 2 * width + kz * keep_x + kk
                im = re + width
                zf[row, re] = np.cos(a)
                zf[row, im] = -np.sin(a)
                zf[row + keep_x, re] = np.sin(a)
                zf[row + keep_x, im] = np.cos(a)
    zi = np.zeros((2 * width, full * slot))
    for z in range(full):
        a = 2 * math.pi / full * ((kz * z) % full)
        for kk in range(keep_x):
            re = kz * keep_x + kk
            im = re + width
            col = z * slot + kk
            zi[re, col] = np.cos(a)
            zi[im, col] = -np.sin(a)
            zi[re, col + keep_x] = np.sin(a)
            zi[im, col + keep_x] = np.cos(a)
    tz = 2 * math.pi / full * kz
    ty = 2 * math.pi / rows * ky
    tx = 2 * math.pi / cols * k
    live = (ky != -keep_y).astype(np.float64)[:, None, None]
    real = 1.0 + diffusion_number * (
        (2 * np.cos(ty) - 2)[:, None, None]
        + (2 * np.cos(tz) - 2)[None, :, None]
        + (2 * np.cos(tx) - 2)[None, None, :]
    )
    imag = -(
        advect_yaxis * np.sin(ty)[:, None, None]
        + advect_zaxis * np.sin(tz)[None, :, None]
        + advect_xaxis * np.sin(tx)[None, None, :]
    )
    symbol = np.stack([real * live, imag * live]).reshape(2, 2 * keep_y, width)
    return [xf, yf, zf, zi, yi, xi], symbol.astype(np.float32)


def halves(table):
    high = table.astype(jnp.bfloat16)
    low = (table - high.astype(np.float64)).astype(jnp.bfloat16)
    return np.stack([high, low])


def split(values):
    high = values.astype(jnp.bfloat16)
    return high, (values - high.astype(jnp.float32)).astype(jnp.bfloat16)


def dot(a, b):
    return jnp.dot(a, b, preferred_element_type=jnp.float32)


def times(values, table):
    high, low = split(values)
    return dot(high, table[0]) + dot(low, table[0]) + dot(high, table[1])


def under(table, values):
    high, low = split(values)
    return dot(table[0], high) + dot(table[0], low) + dot(table[1], high)


def kernel(
    sizes, starts, source, xf_h, yf_h, zf_h, zi_h, yi_h, xi_h, sym_h,
    ends, slice_out, total_out,
    y1, y2, y3, y4, src, fine, halo, xf, yf, zf, zi, yi, xi, sym,
    own, jumps, ahead, mode_send, mode_recv, square_send, squares,
    load_sem, table_sem, halo_send, halo_recv, ahead_sems, jump_send, jump_recv,
    mode_ssem, mode_rsem, sq_send, sq_recv, out_sem,
):
    times_n, spaces, fields, depth, rows, cols = sizes
    keep_y, keep_x = rows // 8, cols // 16
    slot = 2 * keep_x
    ky = 2 * keep_y
    layers = fields * depth
    slots = LANES // slot
    groups = -(-layers // slots)
    per = LANES // (slot * depth)
    chunks = rows // CHUNK
    devices = times_n * spaces
    n = lax.axis_index("tm")
    s = lax.axis_index("space")
    me = n * spaces + s
    up = lax.rem(s + 1, spaces)
    down = lax.rem(s + spaces - 1, spaces)

    barrier = pltpu.get_barrier_semaphore()

    def greet(i, c):
        @pl.when(i != me)
        def _():
            pl.semaphore_signal(
                barrier, inc=1, device_id=(i // spaces, lax.rem(i, spaces)), device_id_type=MESH
            )

        return c

    lax.fori_loop(0, devices, greet, 0)
    loads = [
        pltpu.make_async_copy(starts.at[0], y1.at[:, :, pl.ds(PAD, rows)], load_sem.at[0]),
        pltpu.make_async_copy(
            starts.at[0, :, :, pl.ds(rows - PAD, PAD)], y1.at[:, :, pl.ds(0, PAD)], load_sem.at[1]
        ),
        pltpu.make_async_copy(
            starts.at[0, :, :, pl.ds(0, PAD)], y1.at[:, :, pl.ds(PAD + rows, PAD)], load_sem.at[2]
        ),
        pltpu.make_async_copy(source, src, load_sem.at[3]),
    ]
    for copy in loads:
        copy.start()
    fills = [
        pltpu.make_async_copy(a, b, table_sem.at[i])
        for i, (a, b) in enumerate(
            [(xf_h, xf), (yf_h, yf), (zf_h, zf), (zi_h, zi), (yi_h, yi), (xi_h, xi), (sym_h, sym)]
        )
    ]
    for copy in fills:
        copy.start()
    for copy in loads:
        copy.wait()
    pl.semaphore_wait(barrier, devices - 1)

    states = [y1, y2, y3, y4]

    def halo_copy(stage, side, chunk):
        r0 = pl.multiple_of(chunk * CHUNK, CHUNK)
        state = states[stage]
        layer = depth - 1 if side == 0 else 0
        return pltpu.make_async_remote_copy(
            src_ref=state.at[:, layer, pl.ds(pl.multiple_of(PAD + r0, 8), CHUNK)],
            dst_ref=halo.at[stage, side, :, pl.ds(r0, CHUNK)],
            send_sem=halo_send.at[stage, side, chunk],
            recv_sem=halo_recv.at[stage, side, chunk],
            device_id=(n, up if side == 0 else down),
            device_id_type=MESH,
        )

    def send_first(c, carry):
        for side in range(2):
            halo_copy(0, side, c).start()
        return carry

    lax.fori_loop(0, chunks, send_first, 0)

    lane = lax.broadcasted_iota(jnp.int32, (1, LANES), 1)
    first = lax.rem(lane, slot) < keep_x

    def swapped(values):
        return jnp.where(
            first, pltpu.roll(values, LANES - keep_x, 1), -pltpu.roll(values, keep_x, 1)
        )

    def transform(layer_of):
        pairs = jnp.concatenate(
            [
                jnp.concatenate([layer_of(2 * p), layer_of(2 * p + 1)], axis=1)
                for p in range(layers // 2)
            ],
            axis=0,
        )
        packed = times(pairs, xf)
        result = []
        for g in range(groups):
            total = None
            for p in range(slots // 2):
                index = g * (slots // 2) + p
                if index < layers // 2:
                    piece = packed[index * rows : (index + 1) * rows]
                    if p > 0:
                        piece = pltpu.roll(piece, 2 * p * slot, 1)
                    total = piece if total is None else total + piece
            result.append(total)
        both = [jnp.concatenate([t, swapped(t)], axis=0) for t in result]
        spec = under(yf, jnp.concatenate(both, axis=1))
        return jnp.concatenate([spec[:, g * LANES : (g + 1) * LANES] for g in range(groups)], axis=0)

    for copy in fills:
        copy.wait()

    own[...] = transform(lambda l: y1[l // depth, l % depth, pl.ds(PAD, rows)])
    ahead_copy = pltpu.make_async_remote_copy(
        src_ref=own,
        dst_ref=ahead,
        send_sem=ahead_sems.at[0],
        recv_sem=ahead_sems.at[1],
        device_id=(jnp.maximum(n - 1, 0), s),
        device_id_type=MESH,
    )

    @pl.when(n > 0)
    def _():
        ahead_copy.start()

    def update(stage, z, r0, below, above):
        state = states[stage]
        mid, xm, xp, ym, yp = [], [], [], [], []
        rolled = CHUNK + 2 * PAD
        for f in range(fields):
            wide = state[f, z, pl.ds(r0, rolled)]
            centre = wide[PAD : PAD + CHUNK]
            mid.append(centre)
            ym.append(pltpu.roll(wide, 1, 0)[PAD : PAD + CHUNK])
            yp.append(pltpu.roll(wide, rolled - 1, 0)[PAD : PAD + CHUNK])
            xm.append(pltpu.roll(centre, 1, 1))
            xp.append(pltpu.roll(centre, cols - 1, 1))
        zm = [below(f) for f in range(fields)]
        zp = [above(f) for f in range(fields)]
        sides = [xm, xp, ym, yp, zm, zp]
        factors = []
        for axis, speed in enumerate((advect_xaxis, advect_yaxis, advect_zaxis)):
            factors.append((viscosity + 0.5 * speed) + 0.5 * sides[2 * axis][axis])
            factors.append((viscosity - 0.5 * speed) - 0.5 * sides[2 * axis + 1][axis])
        shift = viscosity - diffusivity
        rates = []
        for f in range(fields):
            forcing = src[f, z, pl.ds(r0, CHUNK)]
            if f == 3:
                total = (
                    (xp[0] - xm[0]) + (yp[1] - ym[1]) + (zp[2] - zm[2])
                ) * (-0.5 * compress_rate)
            else:
                gain = viscosity if f < 3 else diffusivity
                total = (-6.0 * gain) * mid[f]
                for factor, side in zip(factors, sides):
                    total = total + (factor if f < 3 else factor - shift) * side[f]
                if f < 3:
                    total = total + 0.5 * (sides[2 * f][3] - sides[2 * f + 1][3])
            rates.append(total + forcing)
        share = time_step / 6.0 * (1.0, 2.0, 2.0, 1.0)[stage]
        for f in range(fields):
            at = f * depth + z
            here = pl.ds(r0, CHUNK)
            begin = y1[f, z, pl.ds(pl.multiple_of(r0 + PAD, 8), CHUNK)]
            done = begin if stage == 0 else fine[at, here]
            fine[at, here] = done + share * rates[f]
            if stage < 3:
                later = states[stage + 1]
                step = (0.5, 0.5, 1.0)[stage] * time_step
                value = begin + step * rates[f]
                later[f, z, pl.ds(pl.multiple_of(r0 + PAD, 8), CHUNK)] = value

                @pl.when(r0 == 0)
                def _():
                    later[f, z, pl.ds(PAD + rows, PAD)] = value[:PAD]

                @pl.when(r0 == rows - CHUNK)
                def _():
                    later[f, z, pl.ds(0, PAD)] = value[CHUNK - PAD :]

    for stage in range(4):
        state = states[stage]

        def inner(i, carry):
            z = 1 + i // chunks
            r0 = pl.multiple_of(lax.rem(i, chunks) * CHUNK, CHUNK)
            at = pl.ds(pl.multiple_of(r0 + PAD, 8), CHUNK)
            update(stage, z, r0, lambda f: state[f, z - 1, at], lambda f: state[f, z + 1, at])
            return carry

        def edge(c, carry):
            r0 = pl.multiple_of(c * CHUNK, CHUNK)
            at = pl.ds(pl.multiple_of(r0 + PAD, 8), CHUNK)
            for side in range(2):
                halo_copy(stage, side, c).wait_recv()
                here = lambda f: halo[stage, side, f, pl.ds(r0, CHUNK)]
                if side == 0:
                    update(stage, 0, r0, here, lambda f: state[f, 1, at])
                else:
                    update(stage, depth - 1, r0, lambda f: state[f, depth - 2, at], here)
                if stage < 3:
                    halo_copy(stage + 1, 1 - side, c).start()
            return carry

        lax.fori_loop(0, (depth - 2) * chunks, inner, 0)
        lax.fori_loop(0, chunks, edge, 0)

    spec = transform(lambda l: fine[l])

    @pl.when(n < times_n - 1)
    def _():
        ahead_copy.wait_recv()
        jumps[n] = spec - ahead[...]

    def jump_copy(slot_id, sem_id, target):
        return pltpu.make_async_remote_copy(
            src_ref=jumps.at[slot_id],
            dst_ref=jumps.at[slot_id],
            send_sem=jump_send.at[sem_id],
            recv_sem=jump_recv.at[slot_id],
            device_id=(target, s),
            device_id_type=MESH,
        )

    def send_jump(i, carry):
        target = times_n - 1 - i
        jump_copy(n, target, target).start()
        return carry

    lax.fori_loop(0, times_n - 1 - n, send_jump, 0)

    width = depth * spaces * keep_x
    gain_re = jnp.concatenate([sym[0]] * groups, axis=0)
    gain_im = jnp.concatenate([sym[1]] * groups, axis=0)

    def advance(carry):
        result = []
        for p in range(per):
            re, im = carry[2 * p], carry[2 * p + 1]
            result.append(gain_re * re - gain_im * im)
            result.append(gain_re * im + gain_im * re)
        return result

    def collect(m, carry):
        jump_copy(m, m, n).wait_recv()
        fresh = times(jumps[m], zf)
        return tuple(
            a + fresh[:, i * width : (i + 1) * width] for i, a in enumerate(advance(carry))
        )

    zero = jnp.zeros((groups * ky, width), jnp.float32)
    carry = advance(lax.fori_loop(0, n, collect, (zero,) * (2 * per)))
    stacked = jnp.concatenate(
        [jnp.concatenate([carry[2 * p], carry[2 * p + 1]], axis=1) for p in range(per)], axis=0
    )
    back = times(stacked, zi)
    half = depth * slot
    height = groups * ky

    def piece(offset):
        total = None
        at = offset * half
        tile, inside = at // LANES * LANES, at % LANES
        part = lax.broadcasted_iota(jnp.int32, (1, LANES), 1) // half
        for p in range(per):
            block = back[p * height : (p + 1) * height, tile : tile + LANES]
            move = (p * half - inside) % LANES
            if move:
                block = pltpu.roll(block, move, 1)
            total = block if total is None else jnp.where(part == p, block, total)
        return total

    def mode_copy(offset):
        return pltpu.make_async_remote_copy(
            src_ref=mode_send.at[offset - 1],
            dst_ref=mode_recv.at[offset - 1],
            send_sem=mode_ssem.at[offset - 1],
            recv_sem=mode_rsem.at[offset - 1],
            device_id=(n, lax.rem(s + offset, spaces)),
            device_id_type=MESH,
        )

    for offset in range(1, spaces):
        mode_send[offset - 1] = piece(offset)
        mode_copy(offset).start()
    modes = piece(0)
    for offset in range(1, spaces):
        mode_copy(offset).wait_recv()
        modes = modes + mode_recv[offset - 1]

    weight = jnp.where(lax.rem(lane, keep_x) == 0, 1.0, 2.0)
    scaled = modes * (1.0 / (depth * spaces * rows * cols))
    square = jnp.sum(
        jnp.sum(scaled * scaled * weight, axis=0, keepdims=True), axis=1, keepdims=True
    ) * float(rows * cols)
    square_send[...] = jnp.broadcast_to(square, (1, LANES))
    squares[me] = jnp.broadcast_to(square, (1, LANES))

    def square_copy(index, target):
        return pltpu.make_async_remote_copy(
            src_ref=square_send,
            dst_ref=squares.at[index],
            send_sem=sq_send.at[target],
            recv_sem=sq_recv.at[index],
            device_id=(target // spaces, lax.rem(target, spaces)),
            device_id_type=MESH,
        )

    def send_square(i, carry):
        @pl.when(i != me)
        def _():
            square_copy(me, i).start()

        return carry

    lax.fori_loop(0, devices, send_square, 0)

    both = [
        jnp.concatenate([t, swapped(t)], axis=0)
        for t in (modes[g * ky : (g + 1) * ky] for g in range(groups))
    ]
    planes = under(yi, jnp.concatenate(both, axis=1))
    outs = []
    for g in range(groups):
        plane = planes[:, g * LANES : (g + 1) * LANES]
        count = min(slots, layers - g * slots) // 2
        shifted = [
            plane if p == 0 else pltpu.roll(plane, LANES - 2 * p * slot, 1) for p in range(count)
        ]
        fix = times(jnp.concatenate(shifted, axis=0), xi)
        for p in range(count):
            for i in range(2):
                l = g * slots + 2 * p + i
                fine[l] = fine[l] + fix[p * rows : (p + 1) * rows, i * cols : (i + 1) * cols]
        low = g * slots // depth
        held = 2 * count // depth
        for f in range(low, low + held):
            copy = pltpu.make_async_copy(
                fine.at[pl.ds(f * depth, depth)], ends.at[0, f], out_sem.at[f]
            )
            copy.start()
            outs.append(copy)

    def take_square(i, carry):
        @pl.when(i != me)
        def _():
            square_copy(i, i).wait_recv()

        return carry

    lax.fori_loop(0, devices, take_square, 0)
    cells = fields * depth * spaces * rows * cols
    mine = jnp.sum(squares[pl.ds(n * spaces, spaces)], axis=0)
    every = jnp.sum(squares[...], axis=0)
    slice_out[...] = jnp.sqrt(mine * (1.0 / cells) + epsilon)
    total_out[...] = jnp.sqrt(every * (1.0 / (cells * times_n)) + epsilon)

    def drain_square(i, carry):
        @pl.when(i != me)
        def _():
            square_copy(me, i).wait_send()

        return carry

    lax.fori_loop(0, devices, drain_square, 0)

    def drain_jump(i, carry):
        target = times_n - 1 - i
        jump_copy(n, target, target).wait_send()
        return carry

    lax.fori_loop(0, times_n - 1 - n, drain_jump, 0)

    @pl.when(n > 0)
    def _():
        ahead_copy.wait_send()

    for stage in range(4):

        def drain_halo(c, carry):
            for side in range(2):
                halo_copy(stage, side, c).wait_send()
            return carry

        lax.fori_loop(0, chunks, drain_halo, 0)
    for offset in range(1, spaces):
        mode_copy(offset).wait_send()
    for copy in outs:
        copy.wait()


def solution(mesh):
    times_n, spaces = mesh.shape["tm"], mesh.shape["space"]

    def step(starts, source):
        _, fields, depth, rows, cols = starts.shape
        keep_y, keep_x = rows // 8, cols // 16
        matrices, symbol = tables(depth, rows, cols, spaces)
        constants = [halves(t) for t in matrices] + [symbol]
        ky, slot = 2 * keep_y, 2 * keep_x
        groups = -(-fields * depth // (LANES // slot))
        height = groups * ky
        devices = times_n * spaces
        chunks = rows // CHUNK
        state = pltpu.VMEM((fields, depth, rows + 2 * PAD, cols), jnp.float32)
        dma = pltpu.SemaphoreType.DMA
        ends, slice_row, total_row = pl.pallas_call(
            functools.partial(kernel, (times_n, spaces, fields, depth, rows, cols)),
            out_shape=(
                jax.ShapeDtypeStruct(starts.shape, jnp.float32),
                jax.ShapeDtypeStruct((1, LANES), jnp.float32),
                jax.ShapeDtypeStruct((1, LANES), jnp.float32),
            ),
            in_specs=[pl.BlockSpec(memory_space=pl.ANY)] * (2 + len(constants)),
            out_specs=(
                pl.BlockSpec(memory_space=pl.ANY),
                pl.BlockSpec(memory_space=pltpu.VMEM),
                pl.BlockSpec(memory_space=pltpu.VMEM),
            ),
            scratch_shapes=[
                state, state, state, state,
                pltpu.VMEM((fields, depth, rows, cols), jnp.float32),
                pltpu.VMEM((fields * depth, rows, cols), jnp.float32),
                pltpu.VMEM((4, 2, fields, rows, cols), jnp.float32),
                *[pltpu.VMEM(c.shape, c.dtype) for c in constants],
                pltpu.VMEM((height, LANES), jnp.float32),
                pltpu.VMEM((times_n, height, LANES), jnp.float32),
                pltpu.VMEM((height, LANES), jnp.float32),
                pltpu.VMEM((spaces - 1, height, LANES), jnp.float32),
                pltpu.VMEM((spaces - 1, height, LANES), jnp.float32),
                pltpu.VMEM((1, LANES), jnp.float32),
                pltpu.VMEM((devices, 1, LANES), jnp.float32),
                dma((4,)), dma((len(constants),)),
                dma((4, 2, chunks)), dma((4, 2, chunks)), dma((2,)),
                dma((times_n,)), dma((times_n,)),
                dma((spaces - 1,)), dma((spaces - 1,)),
                dma((devices,)), dma((devices,)), dma((fields,)),
            ],
            compiler_params=pltpu.CompilerParams(
                collective_id=0, has_side_effects=True, vmem_limit_bytes=48 * 1024 * 1024
            ),
        )(starts, source, *[jnp.asarray(c) for c in constants])
        return ends, slice_row[0, :1], total_row[0, :1]

    return jax.shard_map(
        step,
        mesh=mesh,
        in_specs=(P("tm", None, "space", None, None), P(None, "space", None, None)),
        out_specs=(P("tm", None, "space", None, None), P("tm"), P()),
        check_vma=False,
    )
```

```python
import functools
import math

import jax
import jax.numpy as jnp
import numpy as np
from jax import lax
from jax.experimental import pallas as pl
from jax.experimental.pallas import tpu as pltpu
from jax.sharding import PartitionSpec as P

viscosity = 0.08
diffusivity = 0.05
compress_rate = 0.25
time_step = 0.5
diffusion_number = 0.08
advect_xaxis = 0.2
advect_yaxis = 0.15
advect_zaxis = 0.1
epsilon = 1e-06
MESH = pl.DeviceIdType.MESH
PAD = 8
CHUNK = 16
LANES = 128


def tables(depth, rows, cols, spaces, steps):
    keep_y, keep_x = rows // 8, cols // 16
    slot = 2 * keep_x
    per = LANES // (slot * depth)
    full = depth * spaces
    k = np.arange(keep_x)
    x = np.arange(cols)
    ax = 2 * math.pi / cols * ((x[:, None] * k[None, :]) % cols)
    weight = np.where(k == 0, 1.0, 2.0) / (full * rows * cols)
    xf = np.zeros((2 * cols, LANES))
    xi = np.zeros((LANES, 2 * cols))
    for i in range(2):
        at = i * slot
        xf[i * cols : (i + 1) * cols, at : at + keep_x] = np.cos(ax)
        xf[i * cols : (i + 1) * cols, at + keep_x : at + slot] = -np.sin(ax)
        xi[at : at + keep_x, i * cols : (i + 1) * cols] = (np.cos(ax) * weight).T
        xi[at + keep_x : at + slot, i * cols : (i + 1) * cols] = (-np.sin(ax) * weight).T
    ky = np.arange(2 * keep_y)
    ky = np.where(ky < keep_y, ky, ky - 2 * keep_y)
    y = np.arange(rows)
    ay = 2 * math.pi / rows * ((ky[:, None] * y[None, :]) % rows)
    yf = np.concatenate([np.cos(ay), np.sin(ay)], axis=1)
    yi = np.concatenate([np.cos(ay).T, -np.sin(ay).T], axis=1)
    kz = np.arange(full)
    width = full * keep_x
    half = depth * slot
    zf = np.zeros((LANES, per * 2 * width))
    for fp in range(per):
        for z in range(depth):
            a = 2 * math.pi / full * ((kz * z) % full)
            for kk in range(keep_x):
                row = fp * half + z * slot + kk
                re = fp * 2 * width + kz * keep_x + kk
                im = re + width
                zf[row, re] = np.cos(a)
                zf[row, im] = -np.sin(a)
                zf[row + keep_x, re] = np.sin(a)
                zf[row + keep_x, im] = np.cos(a)
    zi = np.zeros((2 * width, full * slot))
    for z in range(full):
        a = 2 * math.pi / full * ((kz * z) % full)
        for kk in range(keep_x):
            re = kz * keep_x + kk
            im = re + width
            col = z * slot + kk
            zi[re, col] = np.cos(a)
            zi[im, col] = -np.sin(a)
            zi[re, col + keep_x] = np.sin(a)
            zi[im, col + keep_x] = np.cos(a)
    tz = 2 * math.pi / full * kz
    ty = 2 * math.pi / rows * ky
    tx = 2 * math.pi / cols * k
    live = (ky != -keep_y).astype(np.float64)[:, None, None]
    real = 1.0 + diffusion_number * (
        (2 * np.cos(ty) - 2)[:, None, None]
        + (2 * np.cos(tz) - 2)[None, :, None]
        + (2 * np.cos(tx) - 2)[None, None, :]
    )
    imag = -(
        advect_yaxis * np.sin(ty)[:, None, None]
        + advect_zaxis * np.sin(tz)[None, :, None]
        + advect_xaxis * np.sin(tx)[None, None, :]
    )
    symbol = (real + 1j * imag) * live
    powers = np.stack([symbol**p for p in range(1, max(steps, 2))])
    powers = np.stack([powers.real, powers.imag], axis=1).reshape(-1, 2, 2 * keep_y, width)
    return [xf, yf, zf, zi, yi, xi], powers.astype(np.float32)


def halves(table):
    high = table.astype(jnp.bfloat16)
    low = (table - high.astype(np.float64)).astype(jnp.bfloat16)
    return np.stack([high, low])


def split(values):
    high = values.astype(jnp.bfloat16)
    return high, (values - high.astype(jnp.float32)).astype(jnp.bfloat16)


def dot(a, b):
    return jnp.dot(a, b, preferred_element_type=jnp.float32)


def times(values, table):
    high, low = split(values)
    return dot(high, table[0]) + dot(low, table[0]) + dot(high, table[1])


def under(table, values):
    high, low = split(values)
    return dot(table[0], high) + dot(table[0], low) + dot(table[1], high)


def kernel(
    sizes, starts, source, xf_h, yf_h, zf_h, zi_h, yi_h, xi_h, sym_h,
    fine_out, fix_out, slice_out, total_out,
    y1, y2, y3, y4, src, fine, fixes, halo, xf, yf, zf, zi, yi, xi, sym,
    own, jumps, ahead, mode_send, mode_recv, square_send, squares,
    load_sem, table_sem, halo_send, halo_recv, ahead_sems, jump_send, jump_recv,
    mode_ssem, mode_rsem, sq_send, sq_recv, out_sem, relays,
):
    times_n, spaces, fields, depth, rows, cols = sizes
    keep_y, keep_x = rows // 8, cols // 16
    slot = 2 * keep_x
    ky = 2 * keep_y
    layers = fields * depth
    slots = LANES // slot
    groups = -(-layers // slots)
    per = LANES // (slot * depth)
    chunks = rows // CHUNK
    n = lax.axis_index("tm")
    s = lax.axis_index("space")
    me = n * spaces + s
    up = lax.rem(s + 1, spaces)
    down = lax.rem(s + spaces - 1, spaces)

    barrier = pltpu.get_barrier_semaphore()

    def near(distance, act):
        for side, target in enumerate((n - distance, n + distance)):
            pl.when((target >= 0) & (target < times_n))(functools.partial(act, side, target))

    def enter(target, where):
        pl.semaphore_signal(barrier, inc=1, device_id=(target, where), device_id_type=MESH)

    for offset in range(1, spaces):
        enter(n, lax.rem(s + offset, spaces))
    near(1, lambda side, target: enter(target, s))
    loads = [
        pltpu.make_async_copy(starts.at[0, :, 0], y1.at[:, 0, pl.ds(PAD, rows)], load_sem.at[0]),
        pltpu.make_async_copy(
            starts.at[0, :, depth - 1], y1.at[:, depth - 1, pl.ds(PAD, rows)], load_sem.at[4]
        ),
        pltpu.make_async_copy(
            starts.at[0, :, pl.ds(1, depth - 2)],
            y1.at[:, pl.ds(1, depth - 2), pl.ds(PAD, rows)],
            load_sem.at[5],
        ),
        pltpu.make_async_copy(
            starts.at[0, :, :, pl.ds(rows - PAD, PAD)], y1.at[:, :, pl.ds(0, PAD)], load_sem.at[1]
        ),
        pltpu.make_async_copy(
            starts.at[0, :, :, pl.ds(0, PAD)], y1.at[:, :, pl.ds(PAD + rows, PAD)], load_sem.at[2]
        ),
        pltpu.make_async_copy(source, src, load_sem.at[3]),
    ]
    for copy in loads:
        copy.start()
    fills = [
        pltpu.make_async_copy(a, b, table_sem.at[i])
        for i, (a, b) in enumerate(
            [(xf_h, xf), (yf_h, yf), (zf_h, zf), (zi_h, zi), (yi_h, yi), (xi_h, xi), (sym_h, sym)]
        )
    ]
    for copy in fills:
        copy.start()
    for copy in loads[:2]:
        copy.wait()
    beside = jnp.where(n > 0, 1, 0) + jnp.where(n < times_n - 1, 1, 0)
    pl.semaphore_wait(barrier, spaces - 1 + beside)

    def relay(level):
        near(
            2**level,
            lambda side, target: pl.semaphore_signal(
                relays.at[level, side], inc=1, device_id=(target, s), device_id_type=MESH
            ),
        )

    def heard(level):
        near(2**level, lambda side, target: pl.semaphore_wait(relays.at[level, 1 - side], 1))

    levels = (times_n - 1).bit_length()

    states = [y1, y2, y3, y4]

    def halo_copy(stage, side, chunk):
        r0 = pl.multiple_of(chunk * CHUNK, CHUNK)
        state = states[stage]
        layer = depth - 1 if side == 0 else 0
        return pltpu.make_async_remote_copy(
            src_ref=state.at[:, layer, pl.ds(pl.multiple_of(PAD + r0, 8), CHUNK)],
            dst_ref=halo.at[stage, side, :, pl.ds(r0, CHUNK)],
            send_sem=halo_send.at[stage, side, chunk],
            recv_sem=halo_recv.at[stage, side, chunk],
            device_id=(n, up if side == 0 else down),
            device_id_type=MESH,
        )

    def send_first(c, carry):
        for side in range(2):
            halo_copy(0, side, c).start()
        return carry

    lax.fori_loop(0, chunks, send_first, 0)
    relay(0)

    lane = lax.broadcasted_iota(jnp.int32, (1, LANES), 1)
    first = lax.rem(lane, slot) < keep_x

    def swapped(values):
        return jnp.where(
            first, pltpu.roll(values, LANES - keep_x, 1), -pltpu.roll(values, keep_x, 1)
        )

    def transform(layer_of):
        pairs = jnp.concatenate(
            [
                jnp.concatenate([layer_of(2 * p), layer_of(2 * p + 1)], axis=1)
                for p in range(layers // 2)
            ],
            axis=0,
        )
        packed = times(pairs, xf)
        result = []
        for g in range(groups):
            total = None
            for p in range(slots // 2):
                index = g * (slots // 2) + p
                if index < layers // 2:
                    piece = packed[index * rows : (index + 1) * rows]
                    if p > 0:
                        piece = pltpu.roll(piece, 2 * p * slot, 1)
                    total = piece if total is None else total + piece
            result.append(total)
        both = [jnp.concatenate([t, swapped(t)], axis=0) for t in result]
        spec = under(yf, jnp.concatenate(both, axis=1))
        return jnp.concatenate([spec[:, g * LANES : (g + 1) * LANES] for g in range(groups)], axis=0)

    for copy in loads[2:] + fills:
        copy.wait()

    own[...] = transform(lambda l: y1[l // depth, l % depth, pl.ds(PAD, rows)])
    ahead_copy = pltpu.make_async_remote_copy(
        src_ref=own,
        dst_ref=ahead,
        send_sem=ahead_sems.at[0],
        recv_sem=ahead_sems.at[1],
        device_id=(jnp.maximum(n - 1, 0), s),
        device_id_type=MESH,
    )

    @pl.when(n > 0)
    def _():
        ahead_copy.start()

    def update(stage, z, r0, below, above):
        state = states[stage]
        mid, xm, xp, ym, yp = [], [], [], [], []
        rolled = CHUNK + 2 * PAD
        for f in range(fields):
            wide = state[f, z, pl.ds(r0, rolled)]
            centre = wide[PAD : PAD + CHUNK]
            mid.append(centre)
            ym.append(pltpu.roll(wide, 1, 0)[PAD : PAD + CHUNK])
            yp.append(pltpu.roll(wide, rolled - 1, 0)[PAD : PAD + CHUNK])
            xm.append(pltpu.roll(centre, 1, 1))
            xp.append(pltpu.roll(centre, cols - 1, 1))
        zm = [below(f) for f in range(fields)]
        zp = [above(f) for f in range(fields)]
        sides = [xm, xp, ym, yp, zm, zp]
        factors = []
        for axis, speed in enumerate((advect_xaxis, advect_yaxis, advect_zaxis)):
            factors.append((viscosity + 0.5 * speed) + 0.5 * sides[2 * axis][axis])
            factors.append((viscosity - 0.5 * speed) - 0.5 * sides[2 * axis + 1][axis])
        shift = viscosity - diffusivity
        rates = []
        for f in range(fields):
            forcing = src[f, z, pl.ds(r0, CHUNK)]
            if f == 3:
                total = (
                    (xp[0] - xm[0]) + (yp[1] - ym[1]) + (zp[2] - zm[2])
                ) * (-0.5 * compress_rate)
            else:
                gain = viscosity if f < 3 else diffusivity
                total = (-6.0 * gain) * mid[f]
                for factor, side in zip(factors, sides):
                    total = total + (factor if f < 3 else factor - shift) * side[f]
                if f < 3:
                    total = total + 0.5 * (sides[2 * f][3] - sides[2 * f + 1][3])
            rates.append(total + forcing)
        share = time_step / 6.0 * (1.0, 2.0, 2.0, 1.0)[stage]
        for f in range(fields):
            at = f * depth + z
            here = pl.ds(r0, CHUNK)
            begin = y1[f, z, pl.ds(pl.multiple_of(r0 + PAD, 8), CHUNK)]
            done = begin if stage == 0 else fine[at, here]
            fine[at, here] = done + share * rates[f]
            if stage < 3:
                later = states[stage + 1]
                step = (0.5, 0.5, 1.0)[stage] * time_step
                value = begin + step * rates[f]
                later[f, z, pl.ds(pl.multiple_of(r0 + PAD, 8), CHUNK)] = value

                @pl.when(r0 == 0)
                def _():
                    later[f, z, pl.ds(PAD + rows, PAD)] = value[:PAD]

                @pl.when(r0 == rows - CHUNK)
                def _():
                    later[f, z, pl.ds(0, PAD)] = value[CHUNK - PAD :]

    for stage in range(4):
        state = states[stage]

        def inner(i, carry):
            z = 1 + i // chunks
            r0 = pl.multiple_of(lax.rem(i, chunks) * CHUNK, CHUNK)
            at = pl.ds(pl.multiple_of(r0 + PAD, 8), CHUNK)
            update(stage, z, r0, lambda f: state[f, z - 1, at], lambda f: state[f, z + 1, at])
            return carry

        def edge(c, carry):
            r0 = pl.multiple_of(c * CHUNK, CHUNK)
            at = pl.ds(pl.multiple_of(r0 + PAD, 8), CHUNK)
            for side in range(2):
                halo_copy(stage, side, c).wait_recv()
                here = lambda f: halo[stage, side, f, pl.ds(r0, CHUNK)]
                if side == 0:
                    update(stage, 0, r0, here, lambda f: state[f, 1, at])
                else:
                    update(stage, depth - 1, r0, lambda f: state[f, depth - 2, at], here)
                if stage < 3:
                    halo_copy(stage + 1, 1 - side, c).start()
            return carry

        lax.fori_loop(0, (depth - 2) * chunks, inner, 0)
        lax.fori_loop(0, chunks, edge, 0)
        for level in range(levels):
            if min(level, 2) == stage:
                heard(level)
                if level + 1 < levels:
                    relay(level + 1)

    outs = [pltpu.make_async_copy(fine, fine_out, out_sem.at[0])]
    outs[0].start()
    spec = transform(lambda l: fine[l])

    @pl.when(n < times_n - 1)
    def _():
        ahead_copy.wait_recv()
        jumps[n] = spec - ahead[...]

    def jump_copy(slot_id, sem_id, target):
        return pltpu.make_async_remote_copy(
            src_ref=jumps.at[slot_id],
            dst_ref=jumps.at[slot_id],
            send_sem=jump_send.at[sem_id],
            recv_sem=jump_recv.at[slot_id],
            device_id=(target, s),
            device_id_type=MESH,
        )

    def send_jump(i, carry):
        target = times_n - 1 - i
        jump_copy(n, target, target).start()
        return carry

    lax.fori_loop(0, times_n - 1 - n, send_jump, 0)

    width = depth * spaces * keep_x

    def collect(i, carry):
        m = n - 1 - i
        jump_copy(m, m, n).wait_recv()
        fresh = times(jumps[m], zf)
        gain_re = jnp.concatenate([sym[i, 0]] * groups, axis=0)
        gain_im = jnp.concatenate([sym[i, 1]] * groups, axis=0)
        result = []
        for p in range(per):
            re = fresh[:, 2 * p * width : (2 * p + 1) * width]
            im = fresh[:, (2 * p + 1) * width : (2 * p + 2) * width]
            result.append(carry[2 * p] + (gain_re * re - gain_im * im))
            result.append(carry[2 * p + 1] + (gain_re * im + gain_im * re))
        return tuple(result)

    zero = jnp.zeros((groups * ky, width), jnp.float32)
    carry = lax.fori_loop(0, n, collect, (zero,) * (2 * per))
    stacked = jnp.concatenate(
        [jnp.concatenate([carry[2 * p], carry[2 * p + 1]], axis=1) for p in range(per)], axis=0
    )
    back = times(stacked, zi)
    half = depth * slot
    height = groups * ky

    def piece(offset):
        total = None
        at = offset * half
        tile, inside = at // LANES * LANES, at % LANES
        part = lax.broadcasted_iota(jnp.int32, (1, LANES), 1) // half
        for p in range(per):
            block = back[p * height : (p + 1) * height, tile : tile + LANES]
            move = (p * half - inside) % LANES
            if move:
                block = pltpu.roll(block, move, 1)
            total = block if total is None else jnp.where(part == p, block, total)
        return total

    def mode_copy(offset):
        return pltpu.make_async_remote_copy(
            src_ref=mode_send.at[offset - 1],
            dst_ref=mode_recv.at[offset - 1],
            send_sem=mode_ssem.at[offset - 1],
            recv_sem=mode_rsem.at[offset - 1],
            device_id=(n, lax.rem(s + offset, spaces)),
            device_id_type=MESH,
        )

    for offset in range(1, spaces):
        mode_send[offset - 1] = piece(offset)
        mode_copy(offset).start()
    modes = piece(0)
    for offset in range(1, spaces):
        mode_copy(offset).wait_recv()
        modes = modes + mode_recv[offset - 1]

    weight = jnp.where(lax.rem(lane, keep_x) == 0, 1.0, 2.0)
    scaled = modes * (1.0 / (depth * spaces * rows * cols))
    square = jnp.sum(
        jnp.sum(scaled * scaled * weight, axis=0, keepdims=True), axis=1, keepdims=True
    ) * float(rows * cols)
    square_send[...] = jnp.broadcast_to(square, (1, LANES))
    squares[me] = jnp.broadcast_to(square, (1, LANES))

    def square_copy(index, sem_id, target):
        return pltpu.make_async_remote_copy(
            src_ref=square_send,
            dst_ref=squares.at[index],
            send_sem=sq_send.at[sem_id],
            recv_sem=sq_recv.at[index],
            device_id=target,
            device_id_type=MESH,
        )

    def others(act):
        def body(dt, carry):
            t = n - dt
            t = jnp.where(t < 0, t + times_n, t)
            for ds in range(spaces):
                where = s + ds
                where = jnp.where(where >= spaces, where - spaces, where)
                run = functools.partial(act, dt * spaces + ds, t, where)
                if ds == 0:
                    pl.when(dt > 0)(run)
                else:
                    run()
            return carry

        if times_n <= 8:
            for dt in range(times_n):
                body(dt, 0)
        else:
            lax.fori_loop(0, times_n, body, 0)

    others(lambda k, t, where: square_copy(me, k, (t, where)).start())

    both = [
        jnp.concatenate([t, swapped(t)], axis=0)
        for t in (modes[g * ky : (g + 1) * ky] for g in range(groups))
    ]
    planes = under(yi, jnp.concatenate(both, axis=1))
    for g in range(groups):
        plane = planes[:, g * LANES : (g + 1) * LANES]
        count = min(slots, layers - g * slots) // 2
        shifted = [
            plane if p == 0 else pltpu.roll(plane, LANES - 2 * p * slot, 1) for p in range(count)
        ]
        fix = times(jnp.concatenate(shifted, axis=0), xi)
        for p in range(count):
            for i in range(2):
                l = g * slots + 2 * p + i
                fixes[l] = fix[p * rows : (p + 1) * rows, i * cols : (i + 1) * cols]
        held = pl.ds(g * slots, 2 * count)
        copy = pltpu.make_async_copy(fixes.at[held], fix_out.at[held], out_sem.at[1 + g])
        copy.start()
        outs.append(copy)

    others(
        lambda k, t, where: square_copy(t * spaces + where, k, (t, where)).wait_recv()
    )
    cells = fields * depth * spaces * rows * cols
    mine = jnp.sum(squares[pl.ds(n * spaces, spaces)], axis=0)
    every = jnp.sum(squares[...], axis=0)
    slice_out[0] = jnp.sqrt(mine * (1.0 / cells) + epsilon)[0, 0]
    total_out[0] = jnp.sqrt(every * (1.0 / (cells * times_n)) + epsilon)[0, 0]

    others(lambda k, t, where: square_copy(me, k, (t, where)).wait_send())

    def drain_jump(i, carry):
        target = times_n - 1 - i
        jump_copy(n, target, target).wait_send()
        return carry

    lax.fori_loop(0, times_n - 1 - n, drain_jump, 0)

    @pl.when(n > 0)
    def _():
        ahead_copy.wait_send()

    for stage in range(4):

        def drain_halo(c, carry):
            for side in range(2):
                halo_copy(stage, side, c).wait_send()
            return carry

        lax.fori_loop(0, chunks, drain_halo, 0)
    for offset in range(1, spaces):
        mode_copy(offset).wait_send()
    for copy in outs:
        copy.wait()


def solution(mesh):
    times_n, spaces = mesh.shape["tm"], mesh.shape["space"]

    def step(starts, source):
        _, fields, depth, rows, cols = starts.shape
        keep_y, keep_x = rows // 8, cols // 16
        matrices, symbol = tables(depth, rows, cols, spaces, times_n)
        constants = [halves(t) for t in matrices] + [symbol]
        ky, slot = 2 * keep_y, 2 * keep_x
        groups = -(-fields * depth // (LANES // slot))
        height = groups * ky
        chunks = rows // CHUNK
        devices = times_n * spaces
        state = pltpu.VMEM((fields, depth, rows + 2 * PAD, cols), jnp.float32)
        dma = pltpu.SemaphoreType.DMA
        layer_shape = (fields * depth, rows, cols)
        fine, fix, slice_norm, total_norm = pl.pallas_call(
            functools.partial(kernel, (times_n, spaces, fields, depth, rows, cols)),
            out_shape=(
                jax.ShapeDtypeStruct(layer_shape, jnp.float32),
                jax.ShapeDtypeStruct(layer_shape, jnp.float32),
                jax.ShapeDtypeStruct((1,), jnp.float32),
                jax.ShapeDtypeStruct((1,), jnp.float32),
            ),
            in_specs=[pl.BlockSpec(memory_space=pltpu.HBM)] * (2 + len(constants)),
            out_specs=(
                pl.BlockSpec(memory_space=pl.ANY),
                pl.BlockSpec(memory_space=pl.ANY),
                pl.BlockSpec(memory_space=pltpu.SMEM),
                pl.BlockSpec(memory_space=pltpu.SMEM),
            ),
            scratch_shapes=[
                state, state, state, state,
                pltpu.VMEM((fields, depth, rows, cols), jnp.float32),
                pltpu.VMEM(layer_shape, jnp.float32),
                pltpu.VMEM(layer_shape, jnp.float32),
                pltpu.VMEM((4, 2, fields, rows, cols), jnp.float32),
                *[pltpu.VMEM(c.shape, c.dtype) for c in constants],
                pltpu.VMEM((height, LANES), jnp.float32),
                pltpu.VMEM((times_n, height, LANES), jnp.float32),
                pltpu.VMEM((height, LANES), jnp.float32),
                pltpu.VMEM((spaces - 1, height, LANES), jnp.float32),
                pltpu.VMEM((spaces - 1, height, LANES), jnp.float32),
                pltpu.VMEM((1, LANES), jnp.float32),
                pltpu.VMEM((devices, 1, LANES), jnp.float32),
                dma((6,)), dma((len(constants),)),
                dma((4, 2, chunks)), dma((4, 2, chunks)), dma((2,)),
                dma((times_n,)), dma((times_n,)),
                dma((spaces - 1,)), dma((spaces - 1,)),
                dma((devices,)), dma((devices,)), dma((2 * fields,)),
                pltpu.SemaphoreType.REGULAR(((times_n - 1).bit_length(), 2)),
            ],
            compiler_params=pltpu.CompilerParams(
                collective_id=0, has_side_effects=True, vmem_limit_bytes=67043328
            ),
        )(starts, source, *[jnp.asarray(c) for c in constants])
        return (fine + fix).reshape(starts.shape), slice_norm, total_norm

    return jax.shard_map(
        step,
        mesh=mesh,
        in_specs=(P("tm", None, "space", None, None), P(None, "space", None, None)),
        out_specs=(P("tm", None, "space", None, None), P("tm"), P()),
        check_vma=False,
    )
```
